16 devices in a mesh: tp: 2 (over z), y: 2 (over y), x: 4 (over x, core).
Axes of the slice: x: 2, y: 2, z: 2, core: 2. Of those that a mesh axis runs over, the one named last changes fastest.
Arguments:
- w_up: float32 [4, 2, 1, 1280, 5120], P('x', 'y', None, None, 'tp')
- w_down: float32 [4, 2, 1, 5120, 1280], P('x', 'y', None, 'tp')
- inputs: bfloat16 [4, 2, 3, 4096, 1280], P('x', 'y')
- targets: bfloat16 [4, 2, 3, 4096, 1280], P('x', 'y')
Outputs:
- output 1: float32 [4, 2, 1, 1280, 5120], P('x', 'y', None, None, 'tp')
- output 2: float32 [4, 2, 1, 5120, 1280], P('x', 'y', None, 'tp')
- output 3: bfloat16 [4, 2, 4096, 1280], P('x', 'y')
All inputs are finite; a program needn't handle non-finite values.
Results may differ from the reference program's by a relative error of at most 0.00216668.
Values are sent between devices in bfloat16 or wider.
A program may use at most 1 GiB of HBM per device.

```python
import jax
import jax.numpy as jnp
from jax import lax

GRID_X = 4
GRID_Y = 2
NUM_LAYERS = 1
NUM_STEPS = 3
BATCH_ROWS = 4096
MODEL_DIM = 1280
HIDDEN_DIM = 5120
NORM_EPS = 1e-6
LEARN_RATE = 0.25
TARGET_SHIFT = 6.0
REPLICA_SPREAD = 0.7


def setup_inputs(seed: int = 0) -> dict:
    keys = jax.random.split(jax.random.key(seed), 8)
    grid_shape = (GRID_X, GRID_Y, NUM_LAYERS)
    weight_gain = (1.0 + REPLICA_SPREAD ** 2) ** -0.5
    w_up = (jax.random.normal(keys[0], (NUM_LAYERS, MODEL_DIM, HIDDEN_DIM), jnp.float32)
            + REPLICA_SPREAD * jax.random.normal(keys[1], grid_shape + (MODEL_DIM, HIDDEN_DIM), jnp.float32)) * weight_gain
    w_down = (jax.random.normal(keys[2], (NUM_LAYERS, HIDDEN_DIM, MODEL_DIM), jnp.float32)
              + REPLICA_SPREAD * jax.random.normal(keys[3], grid_shape + (HIDDEN_DIM, MODEL_DIM), jnp.float32)) * weight_gain
    data_shape = (GRID_X, GRID_Y, NUM_STEPS, BATCH_ROWS, MODEL_DIM)
    offset_shape = (GRID_X, GRID_Y, 1, 1, MODEL_DIM)
    inputs = (jax.random.normal(keys[4], offset_shape, jnp.float32)
              + jax.random.normal(keys[5], data_shape, jnp.float32)).astype(jnp.bfloat16)
    targets = (TARGET_SHIFT * jax.random.normal(keys[6], offset_shape, jnp.float32)
               + jax.random.normal(keys[7], data_shape, jnp.float32)).astype(jnp.bfloat16)
    return {"w_up": w_up, "w_down": w_down, "inputs": inputs, "targets": targets}


def rms_norm(state_f32):
    return state_f32 * lax.rsqrt(jnp.mean(state_f32 * state_f32, axis=-1, keepdims=True) + NORM_EPS)


def replica_step(up_w, down_w, input_t, target_t):
    up_scale = MODEL_DIM ** -0.5
    down_scale = HIDDEN_DIM ** -0.5
    up_bf = up_w.astype(jnp.bfloat16)
    down_bf = down_w.astype(jnp.bfloat16)

    def layer_fwd(state, weights):
        up_l, down_l = weights
        state_f32 = state.astype(jnp.float32)
        normed = rms_norm(state_f32).astype(jnp.bfloat16)
        pre_act = jnp.dot(normed, up_l, preferred_element_type=jnp.float32) * up_scale
        hidden = jax.nn.gelu(pre_act).astype(jnp.bfloat16)
        branch = jnp.dot(hidden, down_l, preferred_element_type=jnp.float32) * down_scale
        return (state_f32 + branch).astype(jnp.bfloat16), state

    last_state, layer_inputs = lax.scan(layer_fwd, input_t, (up_bf, down_bf))
    grad_state = (2.0 / BATCH_ROWS) * (last_state.astype(jnp.float32) - target_t.astype(jnp.float32))

    def layer_bwd(grad_state, items):
        up_l, down_l, state = items
        state_f32 = state.astype(jnp.float32)
        normed_f32, rms_back = jax.vjp(rms_norm, state_f32)
        normed = normed_f32.astype(jnp.bfloat16)
        pre_act = jnp.dot(normed, up_l, preferred_element_type=jnp.float32) * up_scale
        hidden_f32, gelu_back = jax.vjp(jax.nn.gelu, pre_act)
        hidden = hidden_f32.astype(jnp.bfloat16)
        grad_out = (grad_state * down_scale).astype(jnp.bfloat16)
        down_grad = jnp.dot(hidden.T, grad_out, preferred_element_type=jnp.float32)
        grad_hidden = jnp.dot(grad_out, down_l.T, preferred_element_type=jnp.float32)
        grad_pre = (gelu_back(grad_hidden)[0] * up_scale).astype(jnp.bfloat16)
        up_grad = jnp.dot(normed.T, grad_pre, preferred_element_type=jnp.float32)
        grad_norm = jnp.dot(grad_pre, up_l.T, preferred_element_type=jnp.float32)
        return grad_state + rms_back(grad_norm)[0], (up_grad, down_grad)

    unused, grads = lax.scan(layer_bwd, grad_state, (up_bf, down_bf, layer_inputs), reverse=True)
    return grads[0], grads[1], last_state


def mix_grid(params):
    sent = params.astype(jnp.bfloat16).astype(jnp.float32)
    total = (params + jnp.roll(sent, 1, axis=0) + jnp.roll(sent, -1, axis=0)
             + jnp.roll(sent, 1, axis=1) + jnp.roll(sent, -1, axis=1))
    return total / 5.0


def reference(w_up, w_down, inputs, targets):
    count = GRID_X * GRID_Y

    def one_step(carry, data):
        up_w, down_w, unused_preds = carry
        input_t, target_t = data
        up_grad, down_grad, preds = lax.map(
            lambda packed: replica_step(*packed),
            (up_w.reshape((count,) + up_w.shape[2:]), down_w.reshape((count,) + down_w.shape[2:]),
             input_t.reshape((count,) + input_t.shape[2:]), target_t.reshape((count,) + target_t.shape[2:])))
        new_up = mix_grid(up_w) - LEARN_RATE * up_grad.reshape(up_w.shape)
        new_down = mix_grid(down_w) - LEARN_RATE * down_grad.reshape(down_w.shape)
        return (new_up, new_down, preds.reshape(input_t.shape)), None

    first = (w_up, w_down, jnp.zeros((GRID_X, GRID_Y, BATCH_ROWS, MODEL_DIM), jnp.bfloat16))
    steps_in = (jnp.moveaxis(inputs, 2, 0), jnp.moveaxis(targets, 2, 0))
    final, unused = lax.scan(one_step, first, steps_in)
    return final[0], final[1], final[2]
```

```python
import functools
import math

import jax
import jax.numpy as jnp
from jax import lax
from jax.experimental import pallas as pl
from jax.experimental.pallas import tpu as pltpu
from jax.sharding import PartitionSpec as P

NORM_EPS = 1e-6
LEARN_RATE = 0.25
TILE = 512
ROWS = 512
CHUNK = 32
GELU_C = math.sqrt(2.0 / math.pi)
GELU_A = 0.044715
BF = jnp.bfloat16
F32 = jnp.float32
MESH = pl.DeviceIdType.MESH
NT_DIMS = (((1,), (1,)), ((), ()))
MATE, FAR, SIDE, DEEP = 0, 1, 2, 3


def dot_nt(a, b):
    return lax.dot_general(a, b, NT_DIMS, preferred_element_type=F32)


def dot_nn(a, b):
    return jnp.dot(a, b, preferred_element_type=F32)


def kernel(steps, num_rows, hidden, up_scale, down_scale,
           inp, tgt, w1, w2, wb0,
           o1, o2, hb, wb, hs, gm, gf, gy, zr, xin,
           r_v, go_v, v, wt, gb, ob, st,
           s_snd, s_rcv, f_snd, h_snd, h_rcv, x_snd, x_rcv,
           l_wt, l_own, l_g, l_st, l_out):
    half_rows = num_rows // 2
    nt = hidden // TILE
    nb = num_rows // ROWS
    hb_n = half_rows // ROWS
    bufs = (gm, gf, gy, zr)

    ix, iy, iz = lax.axis_index("x"), lax.axis_index("y"), lax.axis_index("tp")
    core = lax.rem(ix, 2)
    host = core == iz
    guest = core != iz
    mate_x = ix + 1 - 2 * core
    mate = {"x": mate_x, "y": iy, "tp": iz}
    far = {"x": 3 - ix, "y": iy, "tp": iz}
    side = {"x": ix, "y": 1 - iy, "tp": iz}
    deep = {"x": ix, "y": iy, "tp": 1 - iz}
    diag = {"x": mate_x, "y": iy, "tp": 1 - iz}
    peers = (mate, far, side, deep)

    barrier = pltpu.get_barrier_semaphore()
    for peer in (mate, far, side, deep, diag):
        pl.semaphore_signal(barrier, inc=1, device_id=peer, device_id_type=MESH)
    pl.semaphore_wait(barrier, 5)

    def tile_rows(j):
        return pl.ds(pl.multiple_of(j * TILE, TILE), TILE)

    def block(m):
        return pl.ds(pl.multiple_of(m * ROWS, ROWS), ROWS)

    def tile_copy(kind, t, j, src):
        return pltpu.make_async_remote_copy(
            src_ref=src.at[:, tile_rows(j)], dst_ref=bufs[kind].at[t, :, tile_rows(j)],
            send_sem=s_snd.at[kind, t, j], recv_sem=s_rcv.at[kind, t, j],
            device_id=peers[kind], device_id_type=MESH)

    def send_tile(t, j, src):
        @pl.when(guest)
        def _():
            tile_copy(DEEP, t, j, src).start()
        for kind in (MATE, FAR, SIDE):
            tile_copy(kind, t, j, src).start()

    def forward_copy(t, j):
        return pltpu.make_async_remote_copy(
            src_ref=zr.at[t, :, tile_rows(j)], dst_ref=zr.at[t, :, tile_rows(j)],
            send_sem=f_snd.at[t, j], recv_sem=s_rcv.at[DEEP, t, j],
            device_id=mate, device_id_type=MESH)

    def half_copy(t):
        other = pl.ds(pl.multiple_of((1 - core) * half_rows, half_rows), half_rows)
        return pltpu.make_async_remote_copy(
            src_ref=inp.at[t, other], dst_ref=xin.at[t], send_sem=x_snd.at[t], recv_sem=x_rcv.at[t],
            device_id=mate, device_id_type=MESH)

    def rows_of(half, m):
        return pl.ds(pl.multiple_of(half * half_rows + m * ROWS, ROWS), ROWS)

    def h_host_copy(t, m):
        return pltpu.make_async_remote_copy(
            src_ref=hb.at[t, rows_of(core, m)], dst_ref=hb.at[t, rows_of(core, m)],
            send_sem=h_snd.at[0, t, m], recv_sem=h_rcv.at[core, t, m], device_id=deep, device_id_type=MESH)

    def h_guest_copy(which, t, m):
        return pltpu.make_async_remote_copy(
            src_ref=hs.at[t, block(m)], dst_ref=hb.at[t, rows_of(core, m)],
            send_sem=h_snd.at[which, t, m], recv_sem=h_rcv.at[core, t, m],
            device_id=(diag, mate)[which], device_id_type=MESH)

    def h_wait(t, half, m):
        pltpu.make_async_remote_copy(
            src_ref=hb.at[t, rows_of(half, m)], dst_ref=hb.at[t, rows_of(half, m)],
            send_sem=h_snd.at[0, t, m], recv_sem=h_rcv.at[half, t, m], device_id=deep, device_id_type=MESH).wait_recv()

    def own_tile(t, j, slot):
        @pl.when(t == 0)
        def _():
            pltpu.make_async_copy(wb0.at[:, tile_rows(j)], wt.at[slot], l_wt.at[slot]).start()

        @pl.when(t > 0)
        def _():
            pltpu.make_async_copy(wb.at[t - 1, :, tile_rows(j)], wt.at[slot], l_wt.at[slot]).start()

    def wait_tile(slot):
        pltpu.make_async_copy(wb0.at[:, tile_rows(0)], wt.at[slot], l_wt.at[slot]).wait()

    def stage(src, slot):
        return pltpu.make_async_copy(src, st.at[slot], l_st.at[slot])

    def stage_wait(slot):
        stage(inp.at[0, block(0)], slot).wait()

    def stage_fwd_rows(t, m, slot):
        @pl.when(host)
        def _():
            stage(inp.at[t, rows_of(core, m)], slot).start()

        @pl.when(guest)
        def _():
            stage(xin.at[t, block(m)], slot).start()

    def norm_block(slot, m):
        def body(c, carry):
            x = st[slot, pl.ds(pl.multiple_of(c * CHUNK, CHUNK), CHUNK), :].astype(F32)
            inv = lax.rsqrt(jnp.mean(x * x, axis=-1, keepdims=True) + NORM_EPS)
            r_v[pl.ds(pl.multiple_of(m * ROWS + c * CHUNK, CHUNK), CHUNK), :] = (x * inv).astype(BF)
            return carry
        lax.fori_loop(0, ROWS // CHUNK, body, 0)

    def zero(first, count):
        def body(c, carry):
            v[pl.ds(pl.multiple_of(first + c * CHUNK, CHUNK), CHUNK), :] = jnp.zeros((CHUNK, v.shape[1]), F32)
            return carry
        lax.fori_loop(0, count // CHUNK, body, 0)

    @pl.when(host)
    def _():
        half_copy(0).start()

    def first_sends(j, carry):
        send_tile(0, j, wb0)
        return carry
    lax.fori_loop(0, nt, first_sends, 0)

    @pl.when(host)
    def _():
        def body(t, carry):
            half_copy(t).start()
            return carry
        lax.fori_loop(1, steps, body, 0)

    def step(t, carry):
        @pl.when(guest)
        def _():
            half_copy(t).wait_recv()
        stage_fwd_rows(t, 0, 0)
        for m in range(hb_n):
            if m + 1 < hb_n:
                stage_fwd_rows(t, m + 1, (m + 1) % 2)
            stage_wait(m % 2)
            norm_block(m % 2, m)
        zero(0, half_rows)

        def start_tile(i, slot):
            j = lax.rem(i, nt)

            @pl.when(jnp.logical_and(i < nt, host))
            def _():
                own_tile(t, j, slot)

            @pl.when(jnp.logical_and(i < nt, guest))
            def _():
                tile_copy(MATE, t, j, wb0).wait_recv()
                pltpu.make_async_copy(gm.at[t, :, tile_rows(j)], wt.at[slot], l_wt.at[slot]).start()

            @pl.when(i >= nt)
            def _():
                tile_copy(DEEP, t, j, wb0).wait_recv()
                pltpu.make_async_copy(zr.at[t, :, tile_rows(j)], wt.at[slot], l_wt.at[slot]).start()

            @pl.when(jnp.logical_and(i >= nt, host))
            def _():
                forward_copy(t, j).start()

        start_tile(jnp.int32(0), 0)

        def fwd_tile(i, carry):
            slot = lax.rem(i, 2)

            @pl.when(i + 1 < 2 * nt)
            def _():
                start_tile(i + 1, 1 - slot)
            wait_tile(slot)

            def fwd_block(m, carry):
                x = dot_nt(r_v[block(m), :], wt[slot, 0]) * up_scale
                cdf = 0.5 + 0.5 * jnp.tanh(x * (GELU_C + (GELU_C * GELU_A) * (x * x)))
                a = (x * cdf).astype(BF)
                v[block(m), :] += dot_nn(a, wt[slot, 1])
                return carry
            lax.fori_loop(0, hb_n, fwd_block, 0)
            return carry
        lax.fori_loop(0, 2 * nt, fwd_tile, 0)

        stage_fwd_rows(t, 0, 0)
        for m in range(hb_n):
            slot = m % 2
            if m + 1 < hb_n:
                stage_fwd_rows(t, m + 1, 1 - slot)
            stage_wait(slot)

            def add_rows(c, carry):
                rows = pl.ds(pl.multiple_of(c * CHUNK, CHUNK), CHUNK)
                acc = v[pl.ds(pl.multiple_of(m * ROWS + c * CHUNK, CHUNK), CHUNK), :]
                ob[slot, rows, :] = (st[slot, rows, :].astype(F32) + acc * down_scale).astype(BF)
                return carry
            lax.fori_loop(0, ROWS // CHUNK, add_rows, 0)

            @pl.when(host)
            def _():
                out = pltpu.make_async_copy(ob.at[slot], hb.at[t, rows_of(core, m)], l_out.at[2])
                out.start()
                out.wait()
                h_host_copy(t, m).start()

            @pl.when(guest)
            def _():
                out = pltpu.make_async_copy(ob.at[slot], hs.at[t, block(m)], l_out.at[2])
                out.start()
                out.wait()
                h_guest_copy(0, t, m).start()
                h_guest_copy(1, t, m).start()

        stage(inp.at[t, block(0)], 0).start()
        for m in range(nb):
            if m + 1 < nb:
                stage(inp.at[t, block(m + 1)], (m + 1) % 2).start()
            stage_wait(m % 2)
            norm_block(m % 2, m)

        own_tile(t, jnp.int32(0), 0)

        def go_piece(i, carry):
            m = i // 2
            half = lax.rem(core + i, 2)
            rows = rows_of(half, m)
            stage(tgt.at[t, rows], 1).start()

            @pl.when(jnp.logical_or(guest, half != core))
            def _():
                h_wait(t, half, m)
            stage(hb.at[t, rows], 0).start()
            stage_wait(1)
            stage_wait(0)

            def body(c, carry):
                part = pl.ds(pl.multiple_of(c * CHUNK, CHUNK), CHUNK)
                diff = st[0, part, :].astype(F32) - st[1, part, :].astype(F32)
                g = ((2.0 / num_rows) * diff) * down_scale
                go_v[pl.ds(pl.multiple_of(half * half_rows + m * ROWS + c * CHUNK, CHUNK), CHUNK), :] = g.astype(BF)
                return carry
            lax.fori_loop(0, ROWS // CHUNK, body, 0)
            return carry
        lax.fori_loop(0, nb, go_piece, 0)

        def load_own(j):
            @pl.when(t == 0)
            def _():
                pltpu.make_async_copy(w1.at[tile_rows(j)], v.at[pl.ds(2 * TILE, TILE)], l_own.at[0]).start()
                pltpu.make_async_copy(w2.at[tile_rows(j)], v.at[pl.ds(3 * TILE, TILE)], l_own.at[1]).start()

            @pl.when(t > 0)
            def _():
                pltpu.make_async_copy(o1.at[tile_rows(j)], v.at[pl.ds(2 * TILE, TILE)], l_own.at[0]).start()
                pltpu.make_async_copy(o2.at[tile_rows(j)], v.at[pl.ds(3 * TILE, TILE)], l_own.at[1]).start()

        def bwd_tile(j, carry):
            slot = lax.rem(j, 2)

            @pl.when(j + 1 < nt)
            def _():
                own_tile(t, j + 1, 1 - slot)
            load_own(j)
            zero(0, 2 * TILE)
            wait_tile(slot)

            def bwd_block(m, carry):
                r_m = r_v[block(m), :]
                go_m = go_v[block(m), :]
                x = dot_nt(wt[slot, 0], r_m) * up_scale
                dh = dot_nt(wt[slot, 1], go_m)
                x2 = x * x
                th = jnp.tanh(x * (GELU_C + (GELU_C * GELU_A) * x2))
                cdf = 0.5 + 0.5 * th
                slope = cdf + (x * (0.5 * GELU_C + (1.5 * GELU_C * GELU_A) * x2)) * (1.0 - th * th)
                a = (x * cdf).astype(BF)
                dp = ((dh * slope) * up_scale).astype(BF)
                v[pl.ds(TILE, TILE), :] += dot_nn(a, go_m)
                v[pl.ds(0, TILE), :] += dot_nn(dp, r_m)

                @pl.when(m == nb - 2)
                def _():
                    @pl.when(host)
                    def _():
                        tile_copy(MATE, t, j, wb0).wait_recv()
                    tile_copy(FAR, t, j, wb0).wait_recv()
                    tile_copy(SIDE, t, j, wb0).wait_recv()
                    for kind in (MATE, FAR, SIDE):
                        pltpu.make_async_copy(bufs[kind].at[t, :, tile_rows(j)], gb.at[kind], l_g.at[kind]).start()
                return carry
            lax.fori_loop(0, nb, bwd_block, 0)

            for kind in (MATE, FAR, SIDE):
                pltpu.make_async_copy(bufs[kind].at[t, :, tile_rows(j)], gb.at[kind], l_g.at[kind]).wait()
            outs = (o1, o2)
            for w in range(2):
                own_at = (2 + w) * TILE
                pltpu.make_async_copy(outs[w].at[tile_rows(j)], v.at[pl.ds(own_at, TILE)], l_own.at[w]).wait()

                def update(c, carry):
                    part = pl.ds(pl.multiple_of(c * CHUNK, CHUNK), CHUNK)
                    own = pl.ds(pl.multiple_of(own_at + c * CHUNK, CHUNK), CHUNK)
                    grad = v[pl.ds(pl.multiple_of(w * TILE + c * CHUNK, CHUNK), CHUNK), :]
                    total = (v[own, :] + gb[MATE, w, part, :].astype(F32) + gb[FAR, w, part, :].astype(F32)
                             + 2.0 * gb[SIDE, w, part, :].astype(F32))
                    new = total * 0.2 - LEARN_RATE * grad
                    v[own, :] = new
                    ob[w, part, :] = new.astype(BF)
                    return carry
                lax.fori_loop(0, TILE // CHUNK, update, 0)
                pltpu.make_async_copy(v.at[pl.ds(own_at, TILE)], outs[w].at[tile_rows(j)], l_out.at[w]).start()

            @pl.when(t < steps - 1)
            def _():
                copy = pltpu.make_async_copy(ob, wb.at[t, :, tile_rows(j)], l_out.at[2])
                copy.start()
                copy.wait()
                send_tile(t + 1, j, wb.at[t])
            for w in range(2):
                pltpu.make_async_copy(v.at[pl.ds((2 + w) * TILE, TILE)], outs[w].at[tile_rows(j)], l_out.at[w]).wait()
            return carry
        lax.fori_loop(0, nt, bwd_tile, 0)
        return carry
    lax.fori_loop(0, steps, step, 0)

    def drain(t, carry):
        def body(j, carry):
            for kind in (MATE, FAR, SIDE):
                tile_copy(kind, t, j, wb0).wait_send()

            @pl.when(guest)
            def _():
                tile_copy(DEEP, t, j, wb0).wait_send()

            @pl.when(host)
            def _():
                forward_copy(t, j).wait_send()
            return carry
        lax.fori_loop(0, nt, body, 0)

        def h_body(m, carry):
            @pl.when(host)
            def _():
                h_host_copy(t, m).wait_send()

            @pl.when(guest)
            def _():
                h_guest_copy(0, t, m).wait_send()
                h_guest_copy(1, t, m).wait_send()
            return carry
        lax.fori_loop(0, hb_n, h_body, 0)

        @pl.when(host)
        def _():
            half_copy(t).wait_send()
        return carry
    lax.fori_loop(0, steps, drain, 0)


def train(inputs, targets, w1, w2, wb0):
    steps, num_rows, model = inputs.shape
    hidden = w1.shape[0]
    nt = hidden // TILE
    half_rows = num_rows // 2
    hb_n = half_rows // ROWS
    body = functools.partial(kernel, steps, num_rows, hidden, model ** -0.5, (2 * hidden) ** -0.5)
    shard = jax.ShapeDtypeStruct((steps, 2, hidden, model), BF)
    out_shape = (
        jax.ShapeDtypeStruct(w1.shape, F32), jax.ShapeDtypeStruct(w2.shape, F32),
        jax.ShapeDtypeStruct(inputs.shape, BF),
        jax.ShapeDtypeStruct((steps - 1, 2, hidden, model), BF),
        jax.ShapeDtypeStruct((steps, half_rows, model), BF),
        shard, shard, shard, shard,
        jax.ShapeDtypeStruct((steps, half_rows, model), BF))
    any_spec = pl.BlockSpec(memory_space=pl.ANY)
    dma = pltpu.SemaphoreType.DMA
    flops = steps * 12 * num_rows * hidden * model
    return pl.pallas_call(
        body, out_shape=out_shape, in_specs=[any_spec] * 5, out_specs=[any_spec] * len(out_shape),
        scratch_shapes=[
            pltpu.VMEM((num_rows, model), BF), pltpu.VMEM((num_rows, model), BF),
            pltpu.VMEM((half_rows, model), F32),
            pltpu.VMEM((2, 2, TILE, model), BF), pltpu.VMEM((3, 2, TILE, model), BF),
            pltpu.VMEM((2, TILE, model), BF), pltpu.VMEM((2, ROWS, model), BF),
            dma((4, steps, nt)), dma((4, steps, nt)), dma((steps, nt)),
            dma((2, steps, hb_n)), dma((2, steps, hb_n)), dma((steps,)), dma((steps,)),
            dma((2,)), dma((2,)), dma((3,)), dma((2,)), dma((3,)),
        ],
        compiler_params=pltpu.CompilerParams(collective_id=0, has_side_effects=True, vmem_limit_bytes=64000000),
        cost_estimate=pl.CostEstimate(flops=flops, bytes_accessed=600000000, transcendentals=0),
        name="steps",
    )(inputs, targets, w1, w2, wb0)


def solution(mesh):
    up_spec = P("x", "y", None, None, "tp")
    down_spec = P("x", "y", None, "tp", None)
    data_spec = P("x", "y")

    def device_fn(up_block, down_block, input_block, target_block):
        w1 = up_block[0, 0, 0].T
        w2 = down_block[0, 0, 0]
        wb0 = jnp.stack([w1.astype(BF), w2.astype(BF)])
        outs = train(input_block[0, 0], target_block[0, 0], w1, w2, wb0)
        return outs[0].T[None, None, None], outs[1][None, None, None], outs[2][-1][None, None]

    def run(w_up, w_down, inputs, targets):
        return jax.shard_map(device_fn, mesh=mesh, in_specs=(up_spec, down_spec, data_spec, data_spec),
                             out_specs=(up_spec, down_spec, data_spec), check_vma=False)(w_up, w_down, inputs, targets)

    return run
```

```python
import functools
import math

import jax
import jax.numpy as jnp
from jax import lax
from jax.experimental import pallas as pl
from jax.experimental.pallas import tpu as pltpu
from jax.sharding import PartitionSpec as P

NORM_EPS = 1e-6
LEARN_RATE = 0.25
TILE = 512
ROWS = 512
CHUNK = 32
GELU_C = math.sqrt(2.0 / math.pi)
GELU_A = 0.044715
BF = jnp.bfloat16
F32 = jnp.float32
MESH = pl.DeviceIdType.MESH
NT_DIMS = (((1,), (1,)), ((), ()))
MATE, FAR, SIDE, DEEP = 0, 1, 2, 3


def dot_nt(a, b):
    return lax.dot_general(a, b, NT_DIMS, preferred_element_type=F32)


def dot_nn(a, b):
    return jnp.dot(a, b, preferred_element_type=F32)


def kernel(steps, num_rows, hidden, up_scale, down_scale,
           inp, tgt, w1, w2,
           o1, o2, hb, wb, hs, rn, gm, gf, gy, zr, xin,
           acc, wall, own, gb, ob, st, rb,
           s_snd, s_rcv, f_snd, h_snd, h_rcv, x_snd, x_rcv,
           l_wt, l_own, l_g, l_st, l_tg, l_rb, l_out, l_of):
    half_rows = num_rows // 2
    nt = hidden // TILE
    nb = num_rows // ROWS
    hb_n = half_rows // ROWS
    bufs = (gm, gf, gy, zr)

    ix, iy, iz = lax.axis_index("x"), lax.axis_index("y"), lax.axis_index("tp")
    core = lax.rem(ix, 2)
    host = core == iz
    guest = core != iz
    mate_x = ix + 1 - 2 * core
    mate = {"x": mate_x, "y": iy, "tp": iz}
    far = {"x": 3 - ix, "y": iy, "tp": iz}
    side = {"x": ix, "y": 1 - iy, "tp": iz}
    deep = {"x": ix, "y": iy, "tp": 1 - iz}
    diag = {"x": mate_x, "y": iy, "tp": 1 - iz}
    peers = (mate, far, side, deep)

    barrier = pltpu.get_barrier_semaphore()
    for peer in (mate, far, side, deep, diag):
        pl.semaphore_signal(barrier, inc=1, device_id=peer, device_id_type=MESH)
    pl.semaphore_wait(barrier, 5)

    def tile_rows(j):
        return pl.ds(pl.multiple_of(j * TILE, TILE), TILE)

    def block(m):
        return pl.ds(pl.multiple_of(m * ROWS, ROWS), ROWS)

    def tile_copy(kind, t, j, src):
        return pltpu.make_async_remote_copy(
            src_ref=src.at[:, tile_rows(j)], dst_ref=bufs[kind].at[t, :, tile_rows(j)],
            send_sem=s_snd.at[kind, t, j], recv_sem=s_rcv.at[kind, t, j],
            device_id=peers[kind], device_id_type=MESH)

    def send_tile(t, j, src):
        @pl.when(guest)
        def _():
            tile_copy(DEEP, t, j, src).start()
        for kind in (MATE, FAR, SIDE):
            tile_copy(kind, t, j, src).start()

    def forward_copy(t, j):
        return pltpu.make_async_remote_copy(
            src_ref=zr.at[t, :, tile_rows(j)], dst_ref=zr.at[t, :, tile_rows(j)],
            send_sem=f_snd.at[t, j], recv_sem=s_rcv.at[DEEP, t, j],
            device_id=mate, device_id_type=MESH)

    def half_copy(t):
        other = pl.ds(pl.multiple_of((1 - core) * half_rows, half_rows), half_rows)
        return pltpu.make_async_remote_copy(
            src_ref=inp.at[t, other], dst_ref=xin.at[t], send_sem=x_snd.at[t], recv_sem=x_rcv.at[t],
            device_id=mate, device_id_type=MESH)

    def rows_of(half, m):
        return pl.ds(pl.multiple_of(half * half_rows + m * ROWS, ROWS), ROWS)

    def h_host_copy(t, m):
        return pltpu.make_async_remote_copy(
            src_ref=hb.at[t, rows_of(core, m)], dst_ref=hb.at[t, rows_of(core, m)],
            send_sem=h_snd.at[0, t, m], recv_sem=h_rcv.at[core, t, m], device_id=deep, device_id_type=MESH)

    def h_guest_copy(which, t, m):
        return pltpu.make_async_remote_copy(
            src_ref=hs.at[t, block(m)], dst_ref=hb.at[t, rows_of(core, m)],
            send_sem=h_snd.at[which, t, m], recv_sem=h_rcv.at[core, t, m],
            device_id=(diag, mate)[which], device_id_type=MESH)

    def h_wait(t, half, m):
        pltpu.make_async_remote_copy(
            src_ref=hb.at[t, rows_of(half, m)], dst_ref=hb.at[t, rows_of(half, m)],
            send_sem=h_snd.at[0, t, m], recv_sem=h_rcv.at[half, t, m], device_id=deep, device_id_type=MESH).wait_recv()

    def own_tile(t, j, slot):
        pltpu.make_async_copy(wb.at[t, :, tile_rows(j)], wall.at[slot], l_wt.at[slot]).start()

    def wait_tile(slot):
        pltpu.make_async_copy(wb.at[0, :, tile_rows(0)], wall.at[slot], l_wt.at[slot]).wait()

    def stage(src, slot):
        return pltpu.make_async_copy(src, st.at[slot], l_st.at[slot])

    def stage_wait(slot):
        stage(inp.at[0, block(0)], slot).wait()

    def stage_fwd_rows(t, m, slot):
        @pl.when(host)
        def _():
            stage(inp.at[t, rows_of(core, m)], slot).start()

        @pl.when(guest)
        def _():
            stage(xin.at[t, block(m)], slot).start()

    def norm_rows(src, dst, base):
        def body(c, carry):
            part = pl.ds(pl.multiple_of(c * CHUNK, CHUNK), CHUNK)
            x = src[part, :].astype(F32)
            inv = lax.rsqrt(jnp.mean(x * x, axis=-1, keepdims=True) + NORM_EPS)
            dst[pl.ds(pl.multiple_of(base + c * CHUNK, CHUNK), CHUNK), :] = (x * inv).astype(BF)
            return carry
        lax.fori_loop(0, ROWS // CHUNK, body, 0, unroll=4)

    def zero(first, count):
        def body(c, carry):
            acc[pl.ds(pl.multiple_of(first + c * CHUNK, CHUNK), CHUNK), :] = jnp.zeros((CHUNK, acc.shape[1]), F32)
            return carry
        lax.fori_loop(0, count // CHUNK, body, 0)

    @pl.when(host)
    def _():
        half_copy(0).start()

    def first_tile(j, carry):
        load_1 = pltpu.make_async_copy(w1.at[:, tile_rows(j)], acc.at[pl.ds(0, acc.shape[1]), pl.ds(0, TILE)], l_own.at[0])
        load_2 = pltpu.make_async_copy(w2.at[tile_rows(j)], own.at[1], l_own.at[1])
        load_1.start()
        load_2.start()
        load_1.wait()
        for c in range(TILE // 128):
            turned = acc[0:acc.shape[1], c * 128:(c + 1) * 128].T
            own[0, c * 128:(c + 1) * 128, :] = turned
            ob[0, c * 128:(c + 1) * 128, :] = turned.astype(BF)
        keep = pltpu.make_async_copy(own.at[0], o1.at[tile_rows(j)], l_out.at[0])
        keep.start()
        load_2.wait()

        def cast(c, carry):
            part = pl.ds(pl.multiple_of(c * CHUNK, CHUNK), CHUNK)
            ob[1, part, :] = own[1, part, :].astype(BF)
            return carry
        lax.fori_loop(0, TILE // CHUNK, cast, 0)
        copy = pltpu.make_async_copy(ob, wb.at[0, :, tile_rows(j)], l_out.at[2])
        copy.start()
        copy.wait()
        send_tile(0, j, wb.at[0])
        keep.wait()
        return carry
    lax.fori_loop(0, nt, first_tile, 0)

    @pl.when(host)
    def _():
        def body(t, carry):
            half_copy(t).start()
            return carry
        lax.fori_loop(1, steps, body, 0)

    blocks = steps * nb

    def pre_stage(n, slot):
        stage(inp.at[n // nb, block(lax.rem(n, nb))], slot).start()

    def pre_keep(n, slot):
        return pltpu.make_async_copy(ob.at[slot], rn.at[n // nb, block(lax.rem(n, nb))], l_out.at[slot])

    pre_stage(jnp.int32(0), 0)

    def pre_norm(n, carry):
        slot = lax.rem(n, 2)

        @pl.when(n + 1 < blocks)
        def _():
            pre_stage(n + 1, 1 - slot)
        stage_wait(slot)

        @pl.when(n > 1)
        def _():
            pre_keep(n - 2, slot).wait()
        norm_rows(st.at[slot], ob.at[slot], 0)
        pre_keep(n, slot).start()
        return carry
    lax.fori_loop(0, blocks, pre_norm, 0)
    for n in (blocks - 2, blocks - 1):
        pre_keep(jnp.int32(n), n % 2).wait()

    def step(t, carry):
        @pl.when(guest)
        def _():
            half_copy(t).wait_recv()
        stage_fwd_rows(t, 0, 0)
        for m in range(hb_n):
            if m + 1 < hb_n:
                stage_fwd_rows(t, m + 1, (m + 1) % 2)
            stage_wait(m % 2)
            norm_rows(st.at[m % 2], gb, m * ROWS)
        zero(0, half_rows)

        def start_tile(i, slot):
            j = lax.rem(i, nt)

            @pl.when(jnp.logical_and(i < nt, host))
            def _():
                own_tile(t, j, slot)

            @pl.when(jnp.logical_and(i < nt, guest))
            def _():
                tile_copy(MATE, t, j, wb.at[0]).wait_recv()
                pltpu.make_async_copy(gm.at[t, :, tile_rows(j)], wall.at[slot], l_wt.at[slot]).start()

            @pl.when(i >= nt)
            def _():
                tile_copy(DEEP, t, j, wb.at[0]).wait_recv()
                pltpu.make_async_copy(zr.at[t, :, tile_rows(j)], wall.at[slot], l_wt.at[slot]).start()

            @pl.when(jnp.logical_and(i >= nt, host))
            def _():
                forward_copy(t, j).start()

        start_tile(jnp.int32(0), 0)

        def fwd_block(m, slot):
            x = dot_nt(gb[block(m), :], wall[slot, 0]) * up_scale
            cdf = 0.5 + 0.5 * jnp.tanh(x * (GELU_C + (GELU_C * GELU_A) * (x * x)))
            a = (x * cdf).astype(BF)
            acc[block(m), :] += dot_nn(a, wall[slot, 1])

        def fwd_tile(i, carry):
            slot = lax.rem(i, 2)
            wait_tile(slot)

            def body(m, carry):
                fwd_block(m, slot)

                @pl.when(m == hb_n - 2)
                def _():
                    start_tile(i + 1, 1 - slot)
                return carry
            lax.fori_loop(0, hb_n, body, 0)
            return carry
        lax.fori_loop(0, 2 * nt - 1, fwd_tile, 0)

        last = (2 * nt - 1) % 2
        stage_fwd_rows(t, jnp.int32(0), 0)
        wait_tile(last)

        def last_block(m, carry):
            slot = lax.rem(m, 2)

            @pl.when(m + 1 < hb_n)
            def _():
                stage_fwd_rows(t, m + 1, 1 - slot)
            fwd_block(m, last)
            stage_wait(slot)

            def add_rows(c, carry):
                rows = pl.ds(pl.multiple_of(c * CHUNK, CHUNK), CHUNK)
                branch = acc[pl.ds(pl.multiple_of(m * ROWS + c * CHUNK, CHUNK), CHUNK), :] * down_scale
                ob[slot, rows, :] = (st[slot, rows, :].astype(F32) + branch).astype(BF)
                return carry
            lax.fori_loop(0, ROWS // CHUNK, add_rows, 0)

            @pl.when(host)
            def _():
                out = pltpu.make_async_copy(ob.at[slot], hb.at[t, rows_of(core, m)], l_out.at[2])
                out.start()
                out.wait()
                h_host_copy(t, m).start()

            @pl.when(guest)
            def _():
                out = pltpu.make_async_copy(ob.at[slot], hs.at[t, block(m)], l_out.at[2])
                out.start()
                out.wait()
                h_guest_copy(0, t, m).start()
                h_guest_copy(1, t, m).start()
            return carry
        lax.fori_loop(0, hb_n, last_block, 0)

        def load_all(j, carry):
            own_tile(t, j, j)
            return carry
        lax.fori_loop(0, nt, load_all, 0)

        def piece(i):
            return rows_of(lax.rem(core + i, 2), i // 2)

        def load_target(i):
            slot = lax.rem(i, 2)
            return pltpu.make_async_copy(tgt.at[t, piece(i)], ob.at[slot], l_tg.at[slot])

        def load_input(i):
            slot = lax.rem(i, 2)
            return pltpu.make_async_copy(rn.at[t, piece(i)], rb.at[slot], l_rb.at[slot])

        def load_h(i):
            slot = lax.rem(i, 2)
            return pltpu.make_async_copy(hb.at[t, piece(i)], st.at[slot], l_st.at[slot])

        def await_h(i):
            half = lax.rem(core + i, 2)

            @pl.when(jnp.logical_or(guest, half != core))
            def _():
                h_wait(t, half, i // 2)
            load_h(i).start()

        def load_mix(j):
            @pl.when(host)
            def _():
                tile_copy(MATE, t, j, wb.at[0]).wait_recv()
            tile_copy(FAR, t, j, wb.at[0]).wait_recv()
            tile_copy(SIDE, t, j, wb.at[0]).wait_recv()
            for kind in (MATE, FAR, SIDE):
                for w in range(2):
                    pltpu.make_async_copy(bufs[kind].at[t, w, tile_rows(j)], gb.at[pl.ds((2 * kind + w) * TILE, TILE)],
                                          l_g.at[2 * kind + w]).start()
            pltpu.make_async_copy(o1.at[tile_rows(j)], own.at[0], l_own.at[0]).start()

            @pl.when(t == 0)
            def _():
                pltpu.make_async_copy(w2.at[tile_rows(j)], own.at[1], l_own.at[1]).start()

            @pl.when(t > 0)
            def _():
                pltpu.make_async_copy(o2.at[tile_rows(j)], own.at[1], l_own.at[1]).start()

        def wait_mix():
            for kind in (MATE, FAR, SIDE):
                for w in range(2):
                    pltpu.make_async_copy(bufs[kind].at[t, w, tile_rows(0)], gb.at[pl.ds((2 * kind + w) * TILE, TILE)],
                                          l_g.at[2 * kind + w]).wait()
            for w in range(2):
                pltpu.make_async_copy(w2.at[tile_rows(0)], own.at[w], l_own.at[w]).wait()

        def grad_rows(j, w):
            return pl.ds(pl.multiple_of((2 * j + w) * TILE, TILE), TILE)

        outs = (o1, o2)

        def keep(j, w):
            return pltpu.make_async_copy(acc.at[grad_rows(j, w)], outs[w].at[tile_rows(j)], l_of.at[j, w])

        def send_new(j):
            @pl.when(t < steps - 1)
            def _():
                pltpu.make_async_copy(ob, wb.at[t + 1, :, tile_rows(j)], l_out.at[2]).wait()
                send_tile(t + 1, j, wb.at[t + 1])

        def update_tile(j):
            wait_mix()
            for w in range(2):
                def update(c, carry):
                    part = pl.ds(pl.multiple_of(c * CHUNK, CHUNK), CHUNK)
                    at = pl.ds(pl.multiple_of((2 * j + w) * TILE + c * CHUNK, CHUNK), CHUNK)

                    def mixed(kind):
                        return gb[pl.ds(pl.multiple_of((2 * kind + w) * TILE + c * CHUNK, CHUNK), CHUNK), :].astype(F32)
                    total = own[w, part, :] + mixed(MATE) + mixed(FAR) + 2.0 * mixed(SIDE)
                    new = total * 0.2 - LEARN_RATE * acc[at, :]
                    acc[at, :] = new
                    ob[w, part, :] = new.astype(BF)
                    return carry
                lax.fori_loop(0, TILE // CHUNK, update, 0, unroll=2)
                keep(j, w).start()

            @pl.when(t < steps - 1)
            def _():
                pltpu.make_async_copy(ob, wb.at[t + 1, :, tile_rows(j)], l_out.at[2]).start()

        load_target(jnp.int32(0)).start()
        load_input(jnp.int32(0)).start()
        zero(0, 2 * nt * TILE)
        await_h(jnp.int32(0))

        def arrive(j, carry):
            wait_tile(j)
            return carry
        lax.fori_loop(0, nt, arrive, 0)

        def bwd_block(i, carry):
            slot = lax.rem(i, 2)
            final = i == nb - 1

            @pl.when(i + 1 < nb)
            def _():
                load_target(i + 1).start()
                load_input(i + 1).start()

            @pl.when(i == nb - 2)
            def _():
                load_mix(jnp.int32(0))
            load_input(i).wait()
            load_target(i).wait()
            load_h(i).wait()

            def scale(c, carry):
                part = pl.ds(pl.multiple_of(c * CHUNK, CHUNK), CHUNK)
                diff = st[slot, part, :].astype(F32) - ob[slot, part, :].astype(F32)
                st[slot, part, :] = (((2.0 / num_rows) * diff) * down_scale).astype(BF)
                return carry
            lax.fori_loop(0, ROWS // CHUNK, scale, 0, unroll=4)

            def bwd_tile(j, carry):
                r_m = rb[slot]
                go_m = st[slot]
                x = dot_nt(wall[j, 0], r_m) * up_scale
                dh = dot_nt(wall[j, 1], go_m)
                x2 = x * x
                th = jnp.tanh(x * (GELU_C + (GELU_C * GELU_A) * x2))
                cdf = 0.5 + 0.5 * th
                slope = cdf + (x * (0.5 * GELU_C + (1.5 * GELU_C * GELU_A) * x2)) * (1.0 - th * th)
                a = (x * cdf).astype(BF)
                dp = ((dh * slope) * up_scale).astype(BF)
                acc[grad_rows(j, 1), :] += dot_nn(a, go_m)
                acc[grad_rows(j, 0), :] += dot_nn(dp, r_m)

                @pl.when(jnp.logical_and(j == nt - 2, i + 1 < nb))
                def _():
                    await_h(i + 1)

                @pl.when(final)
                def _():
                    @pl.when(j > 1)
                    def _():
                        send_new(j - 1)
                    update_tile(j)

                    @pl.when(j == 0)
                    def _():
                        send_new(j)

                    @pl.when(j + 1 < nt)
                    def _():
                        load_mix(j + 1)
                return carry
            lax.fori_loop(0, nt, bwd_tile, 0)
            return carry
        lax.fori_loop(0, nb, bwd_block, 0)
        send_new(jnp.int32(nt - 1))

        def kept(j, carry):
            for w in range(2):
                keep(j, w).wait()
            return carry
        lax.fori_loop(0, nt, kept, 0)
        return carry
    lax.fori_loop(0, steps, step, 0)

    def drain(t, carry):
        def body(j, carry):
            for kind in (MATE, FAR, SIDE):
                tile_copy(kind, t, j, wb.at[0]).wait_send()

            @pl.when(guest)
            def _():
                tile_copy(DEEP, t, j, wb.at[0]).wait_send()

            @pl.when(host)
            def _():
                forward_copy(t, j).wait_send()
            return carry
        lax.fori_loop(0, nt, body, 0)

        def h_body(m, carry):
            @pl.when(host)
            def _():
                h_host_copy(t, m).wait_send()

            @pl.when(guest)
            def _():
                h_guest_copy(0, t, m).wait_send()
                h_guest_copy(1, t, m).wait_send()
            return carry
        lax.fori_loop(0, hb_n, h_body, 0)

        @pl.when(host)
        def _():
            half_copy(t).wait_send()
        return carry
    lax.fori_loop(0, steps, drain, 0)


def train(inputs, targets, w1, w2):
    steps, num_rows, model = inputs.shape
    hidden = w2.shape[0]
    nt = hidden // TILE
    half_rows = num_rows // 2
    hb_n = half_rows // ROWS
    body = functools.partial(kernel, steps, num_rows, hidden, model ** -0.5, (2 * hidden) ** -0.5)
    shard = jax.ShapeDtypeStruct((steps, 2, hidden, model), BF)
    out_shape = (
        jax.ShapeDtypeStruct(w2.shape, F32), jax.ShapeDtypeStruct(w2.shape, F32),
        jax.ShapeDtypeStruct(inputs.shape, BF),
        shard,
        jax.ShapeDtypeStruct((steps, half_rows, model), BF),
        jax.ShapeDtypeStruct(inputs.shape, BF),
        shard, shard, shard, shard,
        jax.ShapeDtypeStruct((steps, half_rows, model), BF))
    any_spec = pl.BlockSpec(memory_space=pl.ANY)
    dma = pltpu.SemaphoreType.DMA
    flops = steps * 12 * num_rows * hidden * model
    return pl.pallas_call(
        body, out_shape=out_shape, in_specs=[any_spec] * 4, out_specs=[any_spec] * len(out_shape),
        scratch_shapes=[
            pltpu.VMEM((2 * hidden, model), F32), pltpu.VMEM((nt, 2, TILE, model), BF),
            pltpu.VMEM((2, TILE, model), F32), pltpu.VMEM((6 * TILE, model), BF),
            pltpu.VMEM((2, TILE, model), BF), pltpu.VMEM((2, ROWS, model), BF), pltpu.VMEM((2, ROWS, model), BF),
            dma((4, steps, nt)), dma((4, steps, nt)), dma((steps, nt)),
            dma((2, steps, hb_n)), dma((2, steps, hb_n)), dma((steps,)), dma((steps,)),
            dma((nt,)), dma((2,)), dma((6,)), dma((2,)), dma((2,)), dma((2,)), dma((3,)), dma((nt, 2)),
        ],
        compiler_params=pltpu.CompilerParams(collective_id=0, has_side_effects=True, vmem_limit_bytes=67043328),
        cost_estimate=pl.CostEstimate(flops=flops, bytes_accessed=600000000, transcendentals=0),
        name="steps",
    )(inputs, targets, w1, w2)


def solution(mesh):
    up_spec = P("x", "y", None, None, "tp")
    down_spec = P("x", "y", None, "tp", None)
    data_spec = P("x", "y")

    def device_fn(up_block, down_block, input_block, target_block):
        outs = train(input_block[0, 0], target_block[0, 0], up_block[0, 0, 0], down_block[0, 0, 0])
        return outs[0].T[None, None, None], outs[1][None, None, None], outs[2][-1][None, None]

    def run(w_up, w_down, inputs, targets):
        return jax.shard_map(device_fn, mesh=mesh, in_specs=(up_spec, down_spec, data_spec, data_spec),
                             out_specs=(up_spec, down_spec, data_spec), check_vma=False)(w_up, w_down, inputs, targets)

    return run
```
